32 devices in a mesh: dp: 2 (over z, core), tp: 16 (over x, y).
Axes of the slice: x: 4, y: 4, z: 1, core: 2. Of those that a mesh axis runs over, the one named last changes fastest.
The devices are a block of a 4x4x8 slice.
Arguments:
- x: bfloat16 [128, 3072], P('dp'), parts along dimension 0
- k_cache: bfloat16 [128, 2048, 32, 96], P('dp', None, 'tp'), parts along dimension 0
- v_cache: bfloat16 [128, 2048, 32, 96], P('dp', None, 'tp'), parts along dimension 0
- gain_a: bfloat16 [3072], replicated
- wq: bfloat16 [3072, 3072], P(None, 'tp')
- wo: bfloat16 [3072, 3072], P('tp')
- gain_m: bfloat16 [3072], replicated
- w_gate: bfloat16 [3072, 8192], P(None, 'tp')
- w_up: bfloat16 [3072, 8192], P(None, 'tp')
- w_down: bfloat16 [8192, 3072], P('tp')
Outputs:
- output: bfloat16 [128, 3072], P('dp'), parts along dimension 0
There are 2 independent parts. The reference program is written for one: setup_inputs(seed, part) draws one part's arguments, and reference() takes and returns one part's arrays. A program takes and returns all parts, laid end to end along the dimension named above; an argument that names none is the same for every part.
All inputs are finite; a program needn't handle non-finite values.
Results may differ from the reference program's by a relative error of at most 0.017.
Values are sent between devices in bfloat16 or wider.
A program may use at most 768 MiB of HBM per device.

```python
import jax
import jax.numpy as jnp
from jax import lax

BATCH = 64
CACHE = 2048
D = 3072
HEADS = 32
KV_HEADS = 32
HEAD = 96
FF = 8192
THETA = 10000


def setup_inputs(seed: int = 0, part: int = 0) -> dict:
    kx, kc, kw, kn, kq, ko, km, kg, ku, kd = jax.random.split(jax.random.key(seed), 10)
    kx, kc, kw = (jax.random.fold_in(k, part) for k in (kx, kc, kw))

    def weights(key, rows, columns):
        return jax.random.normal(key, (rows, columns), jnp.float32) * rows**-0.5

    drawn = {
        "x": jax.random.normal(kx, (BATCH, D), jnp.float32),
        "k_cache": 2 * jax.random.normal(kc, (BATCH, CACHE, KV_HEADS, HEAD), jnp.float32),
        "v_cache": 4 * jax.random.normal(kw, (BATCH, CACHE, KV_HEADS, HEAD), jnp.float32),
        "gain_a": 1 + 0.1 * jax.random.normal(kn, (D,), jnp.float32),
        "wq": 2 * weights(kq, D, HEADS * HEAD),
        "wo": weights(ko, HEADS * HEAD, D),
        "gain_m": 1 + 0.1 * jax.random.normal(km, (D,), jnp.float32),
        "w_gate": weights(kg, D, FF),
        "w_up": weights(ku, D, FF),
        "w_down": 2 * weights(kd, FF, D),
    }
    return {k: v.astype(jnp.bfloat16) for k, v in drawn.items()}


def normed(x, gain):
    wide = x.astype(jnp.float32)
    scale = lax.rsqrt(jnp.mean(wide * wide, -1, keepdims=True) + 1e-6)
    return (wide * scale * gain.astype(jnp.float32)).astype(jnp.bfloat16)


def turned(t, place, theta):
    half = t.shape[-1] // 2
    angle = place.astype(jnp.float32)[:, None] * theta ** (-jnp.arange(half, dtype=jnp.float32) / half)
    cos, sin = jnp.cos(angle)[:, None], jnp.sin(angle)[:, None]
    a, b = t[..., :half].astype(jnp.float32), t[..., half:].astype(jnp.float32)
    return jnp.concatenate([a * cos - b * sin, b * cos + a * sin], -1).astype(jnp.bfloat16)


def matmul(a, w):
    return jnp.dot(a, w, preferred_element_type=jnp.float32).astype(jnp.bfloat16)


def einsum(form, a, b):
    return jnp.einsum(form, a.astype(jnp.float32), b.astype(jnp.float32))


def seen_by(a, wq, k_cache, v_cache, head, theta):
    batch, cache, kv_heads = k_cache.shape[:3]
    place = jnp.full((batch,), cache - 1)
    q = turned(matmul(a, wq).reshape(batch, -1, head), place, theta).reshape(batch, kv_heads, -1, head)
    scores = einsum("bgsd,bugd->bgsu", q, k_cache) * head**-0.5
    weights = jax.nn.softmax(scores, -1).astype(jnp.bfloat16)
    return einsum("bgsu,bugd->bgsd", weights, v_cache).astype(jnp.bfloat16).reshape(batch, -1)


def hidden_of(b, w_gate, w_up):
    gate = jnp.dot(b, w_gate, preferred_element_type=jnp.float32)
    up = jnp.dot(b, w_up, preferred_element_type=jnp.float32)
    return (jax.nn.silu(gate) * up).astype(jnp.bfloat16)


def reference(x, k_cache, v_cache, gain_a, wq, wo, gain_m, w_gate, w_up, w_down):
    seen = seen_by(normed(x, gain_a), wq, k_cache, v_cache, HEAD, THETA)
    h = (x.astype(jnp.float32) + jnp.dot(seen, wo, preferred_element_type=jnp.float32)).astype(jnp.bfloat16)
    hidden = hidden_of(normed(h, gain_m), w_gate, w_up)
    return (h.astype(jnp.float32) + jnp.dot(hidden, w_down, preferred_element_type=jnp.float32)).astype(jnp.bfloat16)
```

```python
import functools

import jax
import jax.numpy as jnp
import numpy as np
from jax import lax
from jax.experimental import pallas as pl
from jax.experimental.pallas import tpu as pltpu
from jax.sharding import PartitionSpec as P

HEAD = 96
THETA = 10000
GROUP = 4
CHUNKS = 4
SLOTS = 4
MESH = pl.DeviceIdType.MESH
F32, BF16 = jnp.float32, jnp.bfloat16


def dot(a, b):
    return jnp.dot(a, b, preferred_element_type=F32)


def dot_t(a, b):
    return lax.dot_general(a, b, (((1,), (1,)), ((), ())), preferred_element_type=F32)


def normed(wide, gain):
    scale = lax.rsqrt(jnp.mean(wide * wide, -1, keepdims=True) + 1e-6)
    return (wide * scale * gain).astype(BF16)


def iota(shape, axis):
    return lax.broadcasted_iota(jnp.int32, shape, axis)


def ones_where(mask):
    return jnp.where(mask, 1.0, 0.0).astype(BF16)


def kernel(
    n, x_hbm, k_hbm, v_hbm, ga_ref, wq_hbm, wo_hbm, gm_ref, wg_hbm, wu_hbm, wd_hbm, cos_ref, sin_ref,
    y_hbm,
    x_v, wq_v, wo_v, wg_v, wu_v, wd_v, k_v, v_v, q_all, o_all, tile_m, xb_v,
    t1, r1, h_all, t2, r2, ys,
    sem_x, sem_w, sem_k, sem_v, sem_b, sem_y, s1, q1, sh, qh, s2, q2, sy, qy,
):
    batch, d = x_hbm.shape
    steps = batch // GROUP
    rows = batch // CHUNKS
    per = steps // CHUNKS
    wide = wq_hbm.shape[0]
    heads = wide // HEAD
    fold = GROUP * wide
    rh = rows // 2
    cg = n // 2
    cw = d // cg
    scale = HEAD**-0.5
    me = lax.axis_index("tp")
    mr, mc = lax.div(me, cg), lax.rem(me, cg)

    def peer_of(k):
        return lax.rem(me + k, n)

    barrier = pltpu.get_barrier_semaphore()
    for k in range(1, n):
        pl.semaphore_signal(barrier, inc=1, device_id={"tp": peer_of(k)}, device_id_type=MESH)

    cx = pltpu.make_async_copy(x_hbm, x_v, sem_x)
    cx.start()
    weights = [(wq_hbm, wq_v), (wo_hbm, wo_v), (wg_hbm, wg_v), (wu_hbm, wu_v), (wd_hbm, wd_v)]

    def weight(i):
        return pltpu.make_async_copy(*weights[i], sem_w.at[i])

    weight(0).start()

    def block_of(ref, c):
        return ref.at[pl.ds(pl.multiple_of(rows * c + rh * mr, rh), rh), pl.ds(pl.multiple_of(cw * mc, 128), cw)]

    def xblock(c):
        return pltpu.make_async_copy(block_of(x_hbm, c), xb_v.at[c], sem_b.at[c])

    def fetch(s, src, dst, sem):
        slot = lax.rem(s, SLOTS)
        return pltpu.make_async_copy(
            src.at[pl.ds(pl.multiple_of(s * fold, fold), fold)], dst.at[slot], sem.at[slot]
        )

    for s in range(SLOTS):
        fetch(s, k_hbm, k_v, sem_k).start()
        fetch(s, v_hbm, v_v, sem_v).start()
    for c in range(CHUNKS):
        xblock(c).start()

    col = iota((1, fold), 1)
    inner = col
    for i in range(1, GROUP):
        inner = inner - jnp.where(col >= i * wide, wide, 0)
    within = inner
    for i in range(1, heads):
        within = within - jnp.where(inner >= i * HEAD, HEAD, 0)
    half = HEAD // 2
    partner = jnp.where(within < half, inner + half, inner - half)
    row = iota((wide, fold), 0)
    tile_m[...] = ones_where(row == inner)
    swap_m = ones_where(row == partner)
    cx.wait()
    a = normed(x_v[...].astype(F32), ga_ref[...].astype(F32))
    weight(0).wait()
    q = dot_t(a, wq_v[...]).astype(BF16)
    turned = (dot(q, tile_m[...]) * cos_ref[...] + dot(q, swap_m) * sin_ref[...]).astype(BF16)
    spread = ones_where(iota((batch * heads, batch), 0) // heads == iota((batch * heads, batch), 1))
    place = lax.rem(iota((batch * heads, 1), 0), GROUP * heads) * HEAD
    mine = (col >= place) & (col < place + HEAD)
    q_all[...] = jnp.where(mine, dot(spread, turned), 0.0)

    pl.semaphore_wait(barrier, n - 1)

    def scatter(term, c, t, r, send, recv):
        for o in range(n):
            i, j = o // cg, o % cg
            t[c, o] = term[i * rh : (i + 1) * rh, j * cw : (j + 1) * cw].astype(BF16)
        for k in range(1, n):
            p = peer_of(k)
            pltpu.make_async_remote_copy(
                src_ref=t.at[c, p], dst_ref=r.at[c, k - 1], send_sem=send.at[c], recv_sem=recv.at[c],
                device_id={"tp": p}, device_id_type=MESH,
            ).start()

    def landed(ref, sem):
        pltpu.make_async_copy(ref, ref, sem).wait()

    def total(c, first, t, r):
        acc = t[c, me].astype(F32)
        for k in range(n - 1):
            acc = acc + r[c, k].astype(F32)
        return (first.astype(F32) + acc).astype(BF16)

    def attention(s):
        slot = lax.rem(s, SLOTS)
        at = pl.ds(pl.multiple_of(s * GROUP * heads, GROUP * heads), GROUP * heads)
        fetch(s, k_hbm, k_v, sem_k).wait()
        scores = dot(q_all[at, :].astype(BF16), k_v[slot]) * scale
        e = jnp.exp(scores - jnp.max(scores, -1, keepdims=True))
        w = (e * (1.0 / jnp.sum(e, -1, keepdims=True))).astype(BF16)
        fetch(s, v_hbm, v_v, sem_v).wait()
        o = dot_t(w, v_v[slot])
        first = iota((GROUP * heads, 1), 0) * HEAD
        o_all[at, :] = jnp.where((col >= first) & (col < first + HEAD), o, 0.0)

        @pl.when(s + SLOTS < steps)
        def _():
            fetch(s + SLOTS, k_hbm, k_v, sem_k).start()
            fetch(s + SLOTS, v_hbm, v_v, sem_v).start()

    def project(c):
        at = pl.ds(pl.multiple_of(c * rows * heads, rows * heads), rows * heads)
        folded = dot_t(o_all[at, :].astype(BF16), tile_m[...]).astype(BF16)
        gather = ones_where(iota((rows, rows * heads), 1) // heads == iota((rows, rows * heads), 0))
        seen = dot(gather, folded).astype(BF16)
        scatter(dot(seen, wo_v[...]), c, t1, r1, s1, q1)

    def states(c):
        xblock(c).wait()
        landed(r1.at[c], q1.at[c])
        h_all[c, me] = total(c, xb_v[c], t1, r1)
        for k in range(1, n):
            pltpu.make_async_remote_copy(
                src_ref=h_all.at[c, me], dst_ref=h_all.at[c, me], send_sem=sh.at[c], recv_sem=qh.at[c],
                device_id={"tp": peer_of(k)}, device_id_type=MESH,
            ).start()

    def mlp(c):
        landed(r1.at[c], qh.at[c])
        h = jnp.concatenate(
            [jnp.concatenate([h_all[c, i * cg + j].astype(F32) for j in range(cg)], 1) for i in range(2)], 0
        )
        b = normed(h, gm_ref[...].astype(F32))
        gate = dot(b, wg_v[...])
        up = dot(b, wu_v[...])
        hidden = (jax.nn.silu(gate) * up).astype(BF16)
        scatter(dot(hidden, wd_v[...]), c, t2, r2, s2, q2)

    def outputs(c):
        landed(r2.at[c], q2.at[c])
        ys[c] = total(c, h_all[c, me], t2, r2)
        pltpu.make_async_copy(ys.at[c], block_of(y_hbm, c), sem_y.at[c]).start()
        for k in range(1, n):
            pltpu.make_async_remote_copy(
                src_ref=ys.at[c], dst_ref=block_of(y_hbm, c), send_sem=sy.at[c], recv_sem=qy.at[c],
                device_id={"tp": peer_of(k)}, device_id_type=MESH,
            ).start()

    gap = 3
    stages = (project, states, mlp, outputs)
    lag = gap * (len(stages) - 1)

    def body(s, carry):
        for i in range(1, len(weights)):

            @pl.when(s == i - 1)
            def _(i=i):
                weight(i).start()

        @pl.when(s < steps)
        def _():
            attention(s)

        @pl.when(s == per - 1)
        def _():
            weight(1).wait()

        @pl.when(s == per - 1 + 2 * gap)
        def _():
            for i in range(2, len(weights)):
                weight(i).wait()

        for i, stage in enumerate(stages):
            past = s - (per - 1) - gap * i

            @pl.when((past >= 0) & (past <= per * (CHUNKS - 1)) & (lax.rem(past + per, per) == 0))
            def _(stage=stage, past=past):
                stage(lax.div(past, per))

        return carry

    lax.fori_loop(0, steps + lag, body, 0)

    for c in range(CHUNKS):
        landed(r1.at[c], s1.at[c])
        landed(r1.at[c], sh.at[c])
        landed(r2.at[c], s2.at[c])
        landed(r2.at[c], sy.at[c])
        landed(r2.at[c], qy.at[c])
        pltpu.make_async_copy(ys.at[c], block_of(y_hbm, c), sem_y.at[c]).wait()


def solution(mesh):
    n = mesh.shape["tp"]

    def step(x, k_cache, v_cache, gain_a, wq, wo, gain_m, w_gate, w_up, w_down):
        batch, cache, heads, head = k_cache.shape
        d, wide = wq.shape
        ff = w_gate.shape[1]
        fold = GROUP * wide
        rows = batch // CHUNKS
        block = (rows // 2, d // (n // 2))
        keys = jnp.transpose(k_cache, (0, 2, 3, 1)).reshape(batch * wide, cache)
        values = jnp.transpose(v_cache, (0, 2, 3, 1)).reshape(batch * wide, cache)
        half = head // 2
        angle = (cache - 1) * float(THETA) ** (-np.arange(half) / half)
        cos, sin = np.cos(angle), np.sin(angle)
        cos = np.tile(np.concatenate([cos, cos]), fold // head)[None].astype(np.float32)
        sin = np.tile(np.concatenate([-sin, sin]), fold // head)[None].astype(np.float32)
        hbm, vmem = pl.BlockSpec(memory_space=pl.ANY), pl.BlockSpec(memory_space=pltpu.VMEM)
        dma, per_chunk = pltpu.SemaphoreType.DMA, pltpu.SemaphoreType.DMA((CHUNKS,))
        return pl.pallas_call(
            functools.partial(kernel, n),
            out_shape=jax.ShapeDtypeStruct(x.shape, BF16),
            in_specs=[hbm, hbm, hbm, vmem, hbm, hbm, vmem, hbm, hbm, hbm, vmem, vmem],
            out_specs=hbm,
            scratch_shapes=[
                pltpu.VMEM((batch, d), BF16),
                pltpu.VMEM((wide, d), BF16),
                pltpu.VMEM((wide, d), BF16),
                pltpu.VMEM((d, ff), BF16),
                pltpu.VMEM((d, ff), BF16),
                pltpu.VMEM((ff, d), BF16),
                pltpu.VMEM((SLOTS, fold, cache), BF16),
                pltpu.VMEM((SLOTS, fold, cache), BF16),
                pltpu.VMEM((batch * heads, fold), F32),
                pltpu.VMEM((batch * heads, fold), F32),
                pltpu.VMEM((wide, fold), BF16),
                pltpu.VMEM((CHUNKS, *block), BF16),
                pltpu.VMEM((CHUNKS, n, *block), BF16),
                pltpu.VMEM((CHUNKS, n - 1, *block), BF16),
                pltpu.VMEM((CHUNKS, n, *block), BF16),
                pltpu.VMEM((CHUNKS, n, *block), BF16),
                pltpu.VMEM((CHUNKS, n - 1, *block), BF16),
                pltpu.VMEM((CHUNKS, *block), BF16),
                dma, dma((5,)), dma((SLOTS,)), dma((SLOTS,)), per_chunk, per_chunk,
                *[per_chunk] * 8,
            ],
            compiler_params=pltpu.CompilerParams(
                collective_id=0, has_side_effects=True, vmem_limit_bytes=62 * 2**20
            ),
        )(x, keys, values, gain_a[None], wq.T, wo, gain_m[None], w_gate, w_up, w_down, cos, sin)

    states, cache, columns, rows_of = P("dp", None), P("dp", None, "tp", None), P(None, "tp"), P("tp", None)
    return jax.shard_map(
        step,
        mesh=mesh,
        in_specs=(states, cache, cache, P(None), columns, rows_of, P(None), columns, columns, rows_of),
        out_specs=states,
        check_vma=False,
    )
```

```python
import functools

import jax
import jax.numpy as jnp
import numpy as np
from jax import lax
from jax.experimental import pallas as pl
from jax.experimental.pallas import tpu as pltpu
from jax.sharding import PartitionSpec as P

HEAD = 96
THETA = 10000
GROUP = 4
CHUNKS = 4
SLOTS = 4
MESH = pl.DeviceIdType.MESH
F32, BF16 = jnp.float32, jnp.bfloat16


def dot(a, b):
    return jnp.dot(a, b, preferred_element_type=F32)


def dot_t(a, b):
    return lax.dot_general(a, b, (((1,), (1,)), ((), ())), preferred_element_type=F32)


def normed(wide, gain):
    scale = lax.rsqrt(jnp.mean(wide * wide, -1, keepdims=True) + 1e-6)
    return (wide * scale * gain).astype(BF16)


def iota(shape, axis):
    return lax.broadcasted_iota(jnp.int32, shape, axis)


def ones_where(mask):
    return jnp.where(mask, 1.0, 0.0).astype(BF16)


def kernel(
    n, x_hbm, k_hbm, v_hbm, ga_hbm, wq_hbm, wo_hbm, gm_hbm, wg_hbm, wu_hbm, wd_hbm, cs_hbm,
    y_hbm,
    x_v, ga_v, gm_v, cs_v, wq_v, wo_v, wg_v, wu_v, wd_v, k_v, v_v, q_all, seen_all, xb_v,
    t1, r1, h_all, te, re, tl, rl, ys,
    sem_i, sem_w, sem_k, sem_v, sem_b, sem_y, s1, q1, sh, qh, s2, q2, sy, qy,
):
    batch, d = x_hbm.shape
    steps = batch // GROUP
    rows = batch // CHUNKS
    per = steps // CHUNKS
    early = CHUNKS - 1
    wide = wq_hbm.shape[0]
    heads = wide // HEAD
    fold = GROUP * wide
    rh = rows // 2
    cg = n // 2
    cw = d // cg
    scale = HEAD**-0.5
    me = lax.axis_index("tp")
    mr, mc = lax.div(me, cg), lax.rem(me, cg)

    def peer_of(k):
        return lax.rem(me + k, n)

    first = [
        pltpu.make_async_copy(a, b, sem_i.at[i])
        for i, (a, b) in enumerate([(x_hbm, x_v), (ga_hbm, ga_v), (wq_hbm, wq_v), (cs_hbm, cs_v), (gm_hbm, gm_v)])
    ]
    for copy in first:
        copy.start()
    weights = [(wo_hbm, wo_v), (wg_hbm, wg_v), (wu_hbm, wu_v), (wd_hbm, wd_v)]

    def weight(i):
        return pltpu.make_async_copy(*weights[i], sem_w.at[i])

    def block_of(ref, c):
        return ref.at[pl.ds(pl.multiple_of(rows * c + rh * mr, rh), rh), pl.ds(pl.multiple_of(cw * mc, 128), cw)]

    def xblock(c):
        return pltpu.make_async_copy(block_of(x_hbm, c), xb_v.at[c], sem_b.at[c])

    def fetch(s, src, dst, sem):
        slot = lax.rem(s, SLOTS)
        return pltpu.make_async_copy(
            src.at[pl.ds(pl.multiple_of(s * fold, fold), fold)], dst.at[slot], sem.at[slot]
        )

    for s in range(SLOTS):
        fetch(s, k_hbm, k_v, sem_k).start(priority=1)
        fetch(s, v_hbm, v_v, sem_v).start(priority=1)
    for c in range(CHUNKS):
        xblock(c).start(priority=1)
    weight(0).start(priority=1)

    barrier = pltpu.get_barrier_semaphore()
    for k in range(1, n):
        pl.semaphore_signal(barrier, inc=1, device_id={"tp": peer_of(k)}, device_id_type=MESH)

    col = iota((1, fold), 1)
    inner = col
    for i in range(1, GROUP):
        inner = inner - jnp.where(col >= i * wide, wide, 0)
    within = inner
    for i in range(1, heads):
        within = within - jnp.where(inner >= i * HEAD, HEAD, 0)
    half = HEAD // 2
    partner = jnp.where(within < half, inner + half, inner - half)
    row = iota((wide, fold), 0)
    tile_m, swap_m = ones_where(row == inner), ones_where(row == partner)

    def place(r):
        return lax.rem(r, GROUP) * wide + lax.div(r, GROUP) * HEAD

    def gain_of(ref):
        g = ref[...].astype(F32)
        return jnp.concatenate([g[i : i + 1] for i in range(g.shape[0])], 1)

    first[0].wait()
    first[1].wait()
    a = normed(x_v[...].astype(F32), gain_of(ga_v))
    first[2].wait()
    q = dot_t(a, wq_v[...]).astype(BF16)
    first[3].wait()
    turned = (dot(q, tile_m) * cs_v[0:1] + dot(q, swap_m) * cs_v[1:2]).astype(BF16)
    many = GROUP * heads
    r = iota((batch * heads, batch), 0)
    spread = ones_where(lax.div(r, many) * GROUP + lax.rem(r, GROUP) == iota((batch * heads, batch), 1))
    at = place(lax.rem(iota((batch * heads, 1), 0), many))
    q_all[...] = jnp.where((col >= at) & (col < at + HEAD), dot(spread, turned), 0.0)

    pl.semaphore_wait(barrier, n - 1)

    def send(src, dst, sems, k):
        pltpu.make_async_remote_copy(
            src_ref=src, dst_ref=dst, send_sem=sems[0], recv_sem=sems[1],
            device_id={"tp": peer_of(k)}, device_id_type=MESH,
        ).start()

    def landed(ref, sem):
        pltpu.make_async_copy(ref, ref, sem).wait()

    def cut(term, t):
        for o in range(n):
            i, j = o // cg, o % cg
            for c in range(term.shape[0] // rows):
                t[o, c * rh : (c + 1) * rh] = term[
                    c * rows + i * rh : c * rows + (i + 1) * rh, j * cw : (j + 1) * cw
                ].astype(BF16)

    def scatter(t, r, sems):
        for k in range(1, n):
            send(t.at[peer_of(k)], r.at[k - 1], sems, k)

    def total(first, t, r):
        acc = t[me].astype(F32)
        for k in range(n - 1):
            acc = acc + r[k].astype(F32)
        return (first + acc).astype(BF16)

    def attention(s):
        slot = lax.rem(s, SLOTS)
        at = pl.ds(pl.multiple_of(s * many, many), many)
        fetch(s, k_hbm, k_v, sem_k).wait()
        scores = dot(q_all[at, :].astype(BF16), k_v[slot]) * scale
        e = jnp.exp(scores - jnp.max(scores, -1, keepdims=True))
        w = (e * (1.0 / jnp.sum(e, -1, keepdims=True))).astype(BF16)
        fetch(s, v_hbm, v_v, sem_v).wait()
        o = dot_t(w, v_v[slot])
        start = place(iota((many, 1), 0))
        o = jnp.where((col >= start) & (col < start + HEAD), o, 0.0)
        o = o[:, : fold // 2] + o[:, fold // 2 :]
        o = o + pltpu.roll(o, fold // 4, axis=1)
        seen_all[s] = o[:GROUP, :wide] + o[GROUP:, :wide]

        @pl.when(s + SLOTS < steps)
        def _():
            fetch(s + SLOTS, k_hbm, k_v, sem_k).start(priority=1)
            fetch(s + SLOTS, v_hbm, v_v, sem_v).start(priority=1)

    def project(c):
        seen = jnp.concatenate([seen_all[c * per + i] for i in range(per)], 0).astype(BF16)
        cut(dot(seen, wo_v[...]), t1.at[c])
        scatter(t1.at[c], r1.at[c], (s1.at[c], q1.at[c]))

    def states(c):
        xblock(c).wait()
        landed(r1.at[c], q1.at[c])
        h_all[c, me] = total(xb_v[c].astype(F32), t1.at[c], r1.at[c])
        for k in range(1, n):
            send(h_all.at[c, me], h_all.at[c, me], (sh.at[c], qh.at[c]), k)

    def mlp(chunks, t):
        for c in chunks:
            landed(r1.at[c], qh.at[c])
        h = jnp.concatenate(
            [
                jnp.concatenate([h_all[c, i * cg + j].astype(F32) for j in range(cg)], 1)
                for c in chunks
                for i in range(2)
            ],
            0,
        )
        b = normed(h, gain_of(gm_v))
        gate = dot(b, wg_v[...])
        up = dot(b, wu_v[...])
        hidden = (jax.nn.silu(gate) * up).astype(BF16)
        cut(dot(hidden, wd_v[...]), t)

    def outputs(chunks, t, r, sem):
        landed(r, sem)
        h = jnp.concatenate([h_all[c, me].astype(F32) for c in chunks], 0)
        y = total(h, t, r)
        for i, c in enumerate(chunks):
            ys[c] = y[i * rh : (i + 1) * rh]
        for c in chunks:
            pltpu.make_async_copy(ys.at[c], block_of(y_hbm, c), sem_y.at[c]).start()
            for k in range(1, n):
                send(ys.at[c], block_of(y_hbm, c), (sy.at[c], qy.at[c]), k)

    def body(s, carry):
        attention(s)

        @pl.when(s == steps - SLOTS - 1)
        def _():
            for i in range(1, len(weights)):
                weight(i).start(priority=1)

        @pl.when(s == per - 1)
        def _():
            weight(0).wait()

        @pl.when(lax.rem(s, per) == per - 1)
        def _():
            project(lax.div(s, per))

        @pl.when((s >= per) & (lax.rem(s, per) == per - 2))
        def _():
            states(lax.div(s, per) - 1)

        return carry

    lax.fori_loop(0, steps, body, 0)

    first[4].wait()
    for i in range(1, len(weights)):
        weight(i).wait()
    head, last = list(range(early)), [early]
    mlp(head, te)
    states(early)
    scatter(te, re, (s2.at[0], q2.at[0]))
    mlp(last, tl)
    scatter(tl, rl, (s2.at[1], q2.at[1]))
    outputs(head, te, re, q2.at[0])
    outputs(last, tl, rl, q2.at[1])

    landed(re, s2.at[0])
    landed(rl, s2.at[1])
    for c in range(CHUNKS):
        landed(r1.at[c], s1.at[c])
        landed(r1.at[c], sh.at[c])
        landed(r1.at[c], sy.at[c])
        landed(r1.at[c], qy.at[c])
        pltpu.make_async_copy(ys.at[c], block_of(y_hbm, c), sem_y.at[c]).wait()


def solution(mesh):
    n = mesh.shape["tp"]

    def step(x, k_cache, v_cache, gain_a, wq, wo, gain_m, w_gate, w_up, w_down):
        batch, cache, heads, head = k_cache.shape
        d, wide = wq.shape
        ff = w_gate.shape[1]
        fold = GROUP * wide
        rows = batch // CHUNKS
        block = (rows // 2, d // (n // 2))
        keys = jnp.transpose(k_cache, (0, 2, 3, 1)).reshape(batch * wide, cache)
        values = jnp.transpose(v_cache, (0, 2, 3, 1)).reshape(batch * wide, cache)
        half = head // 2
        angle = (cache - 1) * float(THETA) ** (-np.arange(half) / half)
        cos, sin = np.cos(angle), np.sin(angle)
        turn = np.stack([np.tile([*cos, *cos], fold // head), np.tile([*-sin, *sin], fold // head)]).astype(np.float32)
        hbm = pl.BlockSpec(memory_space=pl.ANY)
        gains = (d // 128, 128)
        dma, per_chunk = pltpu.SemaphoreType.DMA, pltpu.SemaphoreType.DMA((CHUNKS,))
        return pl.pallas_call(
            functools.partial(kernel, n),
            out_shape=jax.ShapeDtypeStruct(x.shape, BF16),
            in_specs=[hbm] * 11,
            out_specs=hbm,
            scratch_shapes=[
                pltpu.VMEM((batch, d), BF16),
                pltpu.VMEM(gains, BF16),
                pltpu.VMEM(gains, BF16),
                pltpu.VMEM((2, fold), F32),
                pltpu.VMEM((wide, d), BF16),
                pltpu.VMEM((wide, d), BF16),
                pltpu.VMEM((d, ff), BF16),
                pltpu.VMEM((d, ff), BF16),
                pltpu.VMEM((ff, d), BF16),
                pltpu.VMEM((SLOTS, fold, cache), BF16),
                pltpu.VMEM((SLOTS, fold, cache), BF16),
                pltpu.VMEM((batch * heads, fold), F32),
                pltpu.VMEM((batch // GROUP, GROUP, wide), F32),
                pltpu.VMEM((CHUNKS, *block), BF16),
                pltpu.VMEM((CHUNKS, n, *block), BF16),
                pltpu.VMEM((CHUNKS, n - 1, *block), BF16),
                pltpu.VMEM((CHUNKS, n, *block), BF16),
                pltpu.VMEM((n, (CHUNKS - 1) * block[0], block[1]), BF16),
                pltpu.VMEM((n - 1, (CHUNKS - 1) * block[0], block[1]), BF16),
                pltpu.VMEM((n, *block), BF16),
                pltpu.VMEM((n - 1, *block), BF16),
                pltpu.VMEM((CHUNKS, *block), BF16),
                dma((5,)), dma((4,)), dma((SLOTS,)), dma((SLOTS,)), per_chunk, per_chunk,
                *[per_chunk] * 4, dma((2,)), dma((2,)), per_chunk, per_chunk,
            ],
            compiler_params=pltpu.CompilerParams(
                collective_id=0, has_side_effects=True, vmem_limit_bytes=62 * 2**20
            ),
        )(x, keys, values, gain_a.reshape(gains), wq.T, wo, gain_m.reshape(gains), w_gate, w_up, w_down, turn)

    states, cache, columns, rows_of = P("dp", None), P("dp", None, "tp", None), P(None, "tp"), P("tp", None)
    return jax.shard_map(
        step,
        mesh=mesh,
        in_specs=(states, cache, cache, P(None), columns, rows_of, P(None), columns, columns, rows_of),
        out_specs=states,
        check_vma=False,
    )
```

```python
import functools
import math

import jax
import jax.numpy as jnp
import numpy as np
from jax import lax
from jax.experimental import pallas as pl
from jax.experimental.pallas import tpu as pltpu
from jax.sharding import PartitionSpec as P

HEAD = 96
THETA = 10000
GROUP = 4
CHUNKS = 4
LEAD = 1
SLOTS = 4
MESH = pl.DeviceIdType.MESH
F32, BF16 = jnp.float32, jnp.bfloat16


def dot(a, b):
    return jnp.dot(a, b, preferred_element_type=F32)


def dot_t(a, b):
    return lax.dot_general(a, b, (((1,), (1,)), ((), ())), preferred_element_type=F32)


def normed(wide, gain):
    scale = lax.rsqrt(jnp.mean(wide * wide, -1, keepdims=True) + 1e-6)
    return (wide * scale * gain).astype(BF16)


def iota(shape, axis):
    return lax.broadcasted_iota(jnp.int32, shape, axis)


def ones_where(mask):
    return jnp.where(mask, 1.0, 0.0).astype(BF16)


def kernel(
    n, x_hbm, k_hbm, v_hbm, ga_hbm, wq_hbm, wo_hbm, gm_hbm, wg_hbm, wu_hbm, wd_hbm, cs_hbm,
    y_hbm,
    x_v, ga_v, gm_v, cs_v, wq_v, wo_v, wg_v, wu_v, wd_v, k_v, v_v, q_all, scores, seen_all, xb_v,
    t1, r1, h_all, t2, r2, ys,
    sem_i, sem_w, sem_k, sem_v, sem_b, sem_y, s1, q1, sh, qh, s2, q2, sy, qy,
):
    batch, d = x_hbm.shape
    steps = batch // GROUP
    rows = batch // CHUNKS
    per = steps // CHUNKS
    early = CHUNKS - 1
    wide = wq_hbm.shape[0]
    heads = wide // HEAD
    fold = GROUP * wide
    rh = rows // 2
    cg = n // 2
    cw = d // cg
    scale = HEAD**-0.5
    me = lax.axis_index("tp")
    mr, mc = lax.div(me, cg), lax.rem(me, cg)

    side = math.isqrt(n)
    away = [min(i, side - i) for i in range(side)]
    moves = sorted(
        ((i, j) for i in range(side) for j in range(side) if i + j), key=lambda m: (-away[m[0]] - away[m[1]], m)
    )
    peers = [
        lax.rem(lax.div(me, side) + i, side) * side + lax.rem(lax.rem(me, side) + j, side) for i, j in moves
    ]

    first = [
        pltpu.make_async_copy(a, b, sem_i.at[i])
        for i, (a, b) in enumerate([(x_hbm, x_v), (ga_hbm, ga_v), (wq_hbm, wq_v), (cs_hbm, cs_v), (gm_hbm, gm_v)])
    ]
    for copy in first:
        copy.start()
    weights = [(wo_hbm, wo_v), (wg_hbm, wg_v), (wu_hbm, wu_v), (wd_hbm, wd_v)]

    def weight(i):
        return pltpu.make_async_copy(*weights[i], sem_w.at[i])

    def block_of(ref, c):
        return ref.at[2 * c + mr, :, pl.ds(pl.multiple_of(cw * mc, 128), cw)]

    x_rows = x_hbm.reshape(batch // rh, rh, d)

    def xblock(c):
        return pltpu.make_async_copy(block_of(x_rows, c), xb_v.at[c], sem_b.at[c])

    def fetch(s, src, dst, sem):
        slot = lax.rem(s, SLOTS)
        return pltpu.make_async_copy(
            src.at[pl.ds(pl.multiple_of(s * fold, fold), fold)], dst.at[slot], sem.at[slot]
        )

    for s in range(SLOTS + LEAD):
        if s < SLOTS:
            fetch(s, k_hbm, k_v, sem_k).start(priority=1)
        if s >= LEAD:
            fetch(s - LEAD, v_hbm, v_v, sem_v).start(priority=1)
    for c in range(CHUNKS):
        xblock(c).start(priority=1)
    weight(0).start(priority=1)

    barrier = pltpu.get_barrier_semaphore()
    for p in peers:
        pl.semaphore_signal(barrier, inc=1, device_id={"tp": p}, device_id_type=MESH)

    col = iota((1, fold), 1)
    inner = col
    for i in range(1, GROUP):
        inner = inner - jnp.where(col >= i * wide, wide, 0)
    within = inner
    for i in range(1, heads):
        within = within - jnp.where(inner >= i * HEAD, HEAD, 0)
    half = HEAD // 2
    partner = jnp.where(within < half, inner + half, inner - half)
    row = iota((wide, fold), 0)
    tile_m, swap_m = ones_where(row == inner), ones_where(row == partner)

    def place(r):
        return lax.rem(r, GROUP) * wide + lax.div(r, GROUP) * HEAD

    def gain_of(ref):
        g = ref[...].astype(F32)
        return jnp.concatenate([g[i : i + 1] for i in range(g.shape[0])], 1)

    first[0].wait()
    first[1].wait()
    a = normed(x_v[...].astype(F32), gain_of(ga_v))
    first[2].wait()
    q = dot_t(a, wq_v[...]).astype(BF16)
    first[3].wait()
    turned = (dot(q, tile_m) * cs_v[0:1] + dot(q, swap_m) * cs_v[1:2]).astype(BF16)
    many = GROUP * heads
    r = iota((batch * heads, batch), 0)
    spread = ones_where(lax.div(r, many) * GROUP + lax.rem(r, GROUP) == iota((batch * heads, batch), 1))
    at = place(lax.rem(iota((batch * heads, 1), 0), many))
    q_all[...] = jnp.where((col >= at) & (col < at + HEAD), dot(spread, turned), 0.0)

    def send(src, dst, sems, peer):
        pltpu.make_async_remote_copy(
            src_ref=src, dst_ref=dst, send_sem=sems[0], recv_sem=sems[1],
            device_id={"tp": peer}, device_id_type=MESH,
        ).start()

    def landed(ref, sem):
        pltpu.make_async_copy(ref, ref, sem).wait()

    def cut(term, chunks, t):
        for a, c in enumerate(chunks):
            for o in range(n):
                i = a * rows + o // cg * rh
                t[c, o] = term[i : i + rh, o % cg * cw : (o % cg + 1) * cw].astype(BF16)

    def scatter(t, r, sems):
        for k, p in enumerate(peers):
            send(t.at[p], r.at[k], sems, p)

    def total(first, t, r):
        acc = t[me].astype(F32)
        for k in range(n - 1):
            acc = acc + r[k].astype(F32)
        return (first + acc).astype(BF16)

    def step_rows(s):
        return pl.ds(pl.multiple_of(s * many, many), many)

    def qk(s):
        scores[lax.rem(s, LEAD + 1)] = dot(q_all[step_rows(s), :].astype(BF16), k_v[lax.rem(s, SLOTS)]) * scale

    def weights_of(s):
        t = scores[lax.rem(s, LEAD + 1)]
        e = jnp.exp(t - jnp.max(t, -1, keepdims=True))
        return (e * (1.0 / jnp.sum(e, -1, keepdims=True))).astype(BF16)

    def pv(s, w):
        o = dot_t(w, v_v[lax.rem(s, SLOTS)])
        start = place(iota((many, 1), 0))
        o = jnp.where((col >= start) & (col < start + HEAD), o, 0.0)
        o = o[:, : fold // 2] + o[:, fold // 2 :]
        o = o + pltpu.roll(o, fold // 4, axis=1)
        seen_all[s] = o[:GROUP, :wide] + o[GROUP:, :wide]

    def keys_in(s):
        return fetch(s, k_hbm, k_v, sem_k)

    def values_in(s):
        return fetch(s, v_hbm, v_v, sem_v)

    def attention(s):
        keys_in(s + LEAD).wait()
        values_in(s).wait()
        w = weights_of(s)
        qk(s + LEAD)
        pv(s, w)

        @pl.when(s + LEAD + SLOTS < steps)
        def _():
            keys_in(s + LEAD + SLOTS).start(priority=1)

        @pl.when(s + SLOTS < steps)
        def _():
            values_in(s + SLOTS).start(priority=1)

    def project(c):
        seen = jnp.concatenate([seen_all[c * per + i] for i in range(per)], 0).astype(BF16)
        cut(dot(seen, wo_v[...]), [c], t1)
        scatter(t1.at[c], r1.at[c], (s1.at[c], q1.at[c]))

    def states(c):
        xblock(c).wait()
        landed(r1.at[c], q1.at[c])
        h_all[c, me] = total(xb_v[c].astype(F32), t1.at[c], r1.at[c])
        for p in peers:
            send(h_all.at[c, me], h_all.at[c, me], (sh.at[c], qh.at[c]), p)

    def mlp(chunks):
        for c in chunks:
            landed(r1.at[c], qh.at[c])
        h = jnp.concatenate(
            [
                jnp.concatenate([h_all[c, i * cg + j].astype(F32) for j in range(cg)], 1)
                for c in chunks
                for i in range(2)
            ],
            0,
        )
        b = normed(h, gain_of(gm_v))
        gate = dot(b, wg_v[...])
        up = dot(b, wu_v[...])
        hidden = (jax.nn.silu(gate) * up).astype(BF16)
        cut(dot(hidden, wd_v[...]), chunks, t2)

    def scatter2(c):
        scatter(t2.at[c], r2.at[c], (s2.at[c], q2.at[c]))

    def outputs(c):
        landed(r2.at[c], q2.at[c])
        ys[c] = total(h_all[c, me].astype(F32), t2.at[c], r2.at[c])
        pltpu.make_async_copy(ys.at[c], block_of(y_hbm, c), sem_y.at[c]).start()
        for p in peers:
            send(ys.at[c], block_of(y_hbm, c), (sy.at[c], qy.at[c]), p)

    def between(s):
        @pl.when(s == steps - SLOTS - 1)
        def _():
            for i in range(1, len(weights)):
                weight(i).start(priority=1)

        @pl.when(s == per - 1)
        def _():
            weight(0).wait()
            pl.semaphore_wait(barrier, n - 1)

        @pl.when(lax.rem(s, per) == per - 1)
        def _():
            project(lax.div(s, per))

        @pl.when((s >= per) & (s < steps - per) & (lax.rem(s, per) == per - 2))
        def _():
            states(lax.div(s, per) - 1)

    def body(s, carry):
        attention(s)
        between(s)
        return carry

    for s in range(LEAD):
        keys_in(s).wait()
        qk(s)
        keys_in(s + SLOTS).start(priority=1)
    lax.fori_loop(0, steps - LEAD, body, 0)
    for s in range(steps - LEAD, steps):
        w = weights_of(s)
        values_in(s).wait()
        pv(s, w)
    project(early)
    states(early - 1)
    first[4].wait()
    for i in range(1, len(weights)):
        weight(i).wait()
    mlp(range(early - 1))
    for c in range(early - 1):
        scatter2(c)
    states(early)
    mlp([early - 1])
    scatter2(early - 1)
    outputs(0)
    mlp([early])
    scatter2(early)
    for c in range(1, CHUNKS):
        outputs(c)

    for c in range(CHUNKS):
        landed(r1.at[c], s1.at[c])
        landed(r1.at[c], sh.at[c])
        landed(r1.at[c], s2.at[c])
        landed(r1.at[c], sy.at[c])
        landed(r1.at[c], qy.at[c])
        pltpu.make_async_copy(ys.at[c], block_of(y_hbm, c), sem_y.at[c]).wait()


def solution(mesh):
    n = mesh.shape["tp"]

    def step(x, k_cache, v_cache, gain_a, wq, wo, gain_m, w_gate, w_up, w_down):
        batch, cache, heads, head = k_cache.shape
        d, wide = wq.shape
        ff = w_gate.shape[1]
        fold = GROUP * wide
        rows = batch // CHUNKS
        block = (rows // 2, d // (n // 2))
        keys = jnp.transpose(k_cache, (0, 2, 3, 1)).reshape(batch * wide, cache)
        values = jnp.transpose(v_cache, (0, 2, 3, 1)).reshape(batch * wide, cache)
        half = head // 2
        angle = (cache - 1) * float(THETA) ** (-np.arange(half) / half)
        cos, sin = np.cos(angle), np.sin(angle)
        turn = np.stack([np.tile([*cos, *cos], fold // head), np.tile([*-sin, *sin], fold // head)]).astype(np.float32)
        hbm = pl.BlockSpec(memory_space=pltpu.HBM)
        gains = (d // 128, 128)
        dma, per_chunk = pltpu.SemaphoreType.DMA, pltpu.SemaphoreType.DMA((CHUNKS,))
        return pl.pallas_call(
            functools.partial(kernel, n),
            out_shape=pltpu.VMEM((batch // block[0], block[0], d), BF16),
            in_specs=[hbm] * 11,
            out_specs=pl.BlockSpec(memory_space=pltpu.VMEM),
            scratch_shapes=[
                pltpu.VMEM((batch, d), BF16),
                pltpu.VMEM(gains, BF16),
                pltpu.VMEM(gains, BF16),
                pltpu.VMEM((2, fold), F32),
                pltpu.VMEM((wide, d), BF16),
                pltpu.VMEM((wide, d), BF16),
                pltpu.VMEM((d, ff), BF16),
                pltpu.VMEM((d, ff), BF16),
                pltpu.VMEM((ff, d), BF16),
                pltpu.VMEM((SLOTS, fold, cache), BF16),
                pltpu.VMEM((SLOTS, fold, cache), BF16),
                pltpu.VMEM((batch * heads, fold), F32),
                pltpu.VMEM((LEAD + 1, GROUP * heads, cache), F32),
                pltpu.VMEM((batch // GROUP, GROUP, wide), F32),
                pltpu.VMEM((CHUNKS, *block), BF16),
                pltpu.VMEM((CHUNKS, n, *block), BF16),
                pltpu.VMEM((CHUNKS, n - 1, *block), BF16),
                pltpu.VMEM((CHUNKS, n, *block), BF16),
                pltpu.VMEM((CHUNKS, n, *block), BF16),
                pltpu.VMEM((CHUNKS, n - 1, *block), BF16),
                pltpu.VMEM((CHUNKS, *block), BF16),
                dma((5,)), dma((4,)), dma((SLOTS,)), dma((SLOTS,)), per_chunk, per_chunk,
                *[per_chunk] * 8,
            ],
            compiler_params=pltpu.CompilerParams(
                collective_id=0, has_side_effects=True, vmem_limit_bytes=60 * 2**20
            ),
        )(x, keys, values, gain_a.reshape(gains), wq.T, wo, gain_m.reshape(gains), w_gate, w_up, w_down, turn).reshape(x.shape)

    states, cache, columns, rows_of = P("dp", None), P("dp", None, "tp", None), P(None, "tp"), P("tp", None)
    return jax.shard_map(
        step,
        mesh=mesh,
        in_specs=(states, cache, cache, P(None), columns, rows_of, P(None), columns, columns, rows_of),
        out_specs=states,
        check_vma=False,
    )
```

```python
import functools
import math

import jax
import jax.numpy as jnp
import numpy as np
from jax import lax
from jax.experimental import pallas as pl
from jax.experimental.pallas import tpu as pltpu
from jax.sharding import PartitionSpec as P

HEAD = 96
THETA = 10000
GROUP = 4
QUARTER = 4
LEAD = 1
SLOTS = 4
MESH = pl.DeviceIdType.MESH
F32, BF16 = jnp.float32, jnp.bfloat16


def dot(a, b):
    return jnp.dot(a, b, preferred_element_type=F32)


def dot_t(a, b):
    return lax.dot_general(a, b, (((1,), (1,)), ((), ())), preferred_element_type=F32)


def normed(wide, gain):
    scale = lax.rsqrt(jnp.mean(wide * wide, -1, keepdims=True) + 1e-6)
    return (wide * scale * gain).astype(BF16)


def iota(shape, axis):
    return lax.broadcasted_iota(jnp.int32, shape, axis)


def ones_where(mask):
    return jnp.where(mask, 1.0, 0.0).astype(BF16)


def kernel(
    n, x_hbm, k_hbm, v_hbm, ga_hbm, wq_hbm, wo_hbm, gm_hbm, wg_hbm, wu_hbm, wd_hbm, cs_hbm,
    y_hbm,
    x_v, ga_v, gm_v, cs_v, wq_v, wo_v, wg_v, wu_v, wd_v, k_v, v_v, q_all, scores, seen_all, xb_v,
    t1, r1, h_all, t2, r2, ys, a1, b1, a2, b2, h_part,
    sem_i, sem_w, sem_k, sem_v, sem_b, sem_y, s1, q1, sh, qh, s2, q2, sy, qy,
    sa1, qa1, sb1, qb1, sa2, qa2, sb2, qb2,
):
    batch, d = x_hbm.shape
    steps = batch // GROUP
    rows = batch // QUARTER
    per = steps // QUARTER
    chunks = QUARTER - 1
    small = rows // 2
    wide = wq_hbm.shape[0]
    heads = wide // HEAD
    fold = GROUP * wide
    rh = rows // 2
    cg = n // 2
    cw = d // cg
    scale = HEAD**-0.5
    me = lax.axis_index("tp")
    mr, mc = lax.div(me, cg), lax.rem(me, cg)

    side = math.isqrt(n)
    my = (lax.div(me, side), lax.rem(me, side))
    away = [min(i, side - i) for i in range(side)]
    moves = sorted(
        ((i, j) for i in range(side) for j in range(side) if i + j), key=lambda m: (-away[m[0]] - away[m[1]], m)
    )
    peers = [
        lax.rem(lax.div(me, side) + i, side) * side + lax.rem(lax.rem(me, side) + j, side) for i, j in moves
    ]

    first = [
        pltpu.make_async_copy(a, b, sem_i.at[i])
        for i, (a, b) in enumerate([(x_hbm, x_v), (ga_hbm, ga_v), (wq_hbm, wq_v), (cs_hbm, cs_v), (gm_hbm, gm_v)])
    ]
    for copy in first:
        copy.start()
    weights = [(wo_hbm, wo_v), (wg_hbm, wg_v), (wu_hbm, wu_v), (wd_hbm, wd_v)]

    def weight(i):
        return pltpu.make_async_copy(*weights[i], sem_w.at[i])

    def block_of(ref, c):
        return ref.at[2 * c + mr, :, pl.ds(pl.multiple_of(cw * mc, 128), cw)]

    x_rows = x_hbm.reshape(batch // rh, rh, d)

    def xblock(c):
        return pltpu.make_async_copy(block_of(x_rows, c), xb_v.at[c], sem_b.at[c])

    def fetch(s, src, dst, sem):
        slot = lax.rem(s, SLOTS)
        return pltpu.make_async_copy(
            src.at[pl.ds(pl.multiple_of(s * fold, fold), fold)], dst.at[slot], sem.at[slot]
        )

    for s in range(SLOTS + LEAD):
        if s < SLOTS:
            fetch(s, k_hbm, k_v, sem_k).start(priority=1)
        if s >= LEAD:
            fetch(s - LEAD, v_hbm, v_v, sem_v).start(priority=1)
    for c in range(chunks):
        xblock(c).start(priority=1)
    weight(0).start(priority=1)

    barrier = pltpu.get_barrier_semaphore()
    for p in peers:
        pl.semaphore_signal(barrier, inc=1, device_id={"tp": p}, device_id_type=MESH)

    col = iota((1, fold), 1)
    inner = col
    for i in range(1, GROUP):
        inner = inner - jnp.where(col >= i * wide, wide, 0)
    within = inner
    for i in range(1, heads):
        within = within - jnp.where(inner >= i * HEAD, HEAD, 0)
    half = HEAD // 2
    partner = jnp.where(within < half, inner + half, inner - half)
    row = iota((wide, fold), 0)
    tile_m, swap_m = ones_where(row == inner), ones_where(row == partner)

    def place(r):
        return lax.rem(r, GROUP) * wide + lax.div(r, GROUP) * HEAD

    def gain_of(ref):
        g = ref[...].astype(F32)
        return jnp.concatenate([g[i : i + 1] for i in range(g.shape[0])], 1)

    first[0].wait()
    first[1].wait()
    a = normed(x_v[...].astype(F32), gain_of(ga_v))
    first[2].wait()
    q = dot_t(a, wq_v[...]).astype(BF16)
    first[3].wait()
    turned = (dot(q, tile_m) * cs_v[0:1] + dot(q, swap_m) * cs_v[1:2]).astype(BF16)
    many = GROUP * heads
    r = iota((batch * heads, batch), 0)
    spread = ones_where(lax.div(r, many) * GROUP + lax.rem(r, GROUP) == iota((batch * heads, batch), 1))
    at = place(lax.rem(iota((batch * heads, 1), 0), many))
    q_all[...] = jnp.where((col >= at) & (col < at + HEAD), dot(spread, turned), 0.0)

    def send(src, dst, sems, peer):
        pltpu.make_async_remote_copy(
            src_ref=src, dst_ref=dst, send_sem=sems[0], recv_sem=sems[1],
            device_id={"tp": peer}, device_id_type=MESH,
        ).start()

    def landed(ref, sem):
        pltpu.make_async_copy(ref, ref, sem).wait()

    def cut(term, cs, t):
        for a, c in enumerate(cs):
            for o in range(n):
                i = a * rows + o // cg * rh
                t[c, o] = term[i : i + rh, o % cg * cw : (o % cg + 1) * cw].astype(BF16)

    def scatter(t, r, sems):
        for k, p in enumerate(peers):
            send(t.at[p], r.at[k], sems, p)

    def total(first, t, r):
        acc = t[me].astype(F32)
        for k in range(n - 1):
            acc = acc + r[k].astype(F32)
        return (first + acc).astype(BF16)

    def step_rows(s):
        return pl.ds(pl.multiple_of(s * many, many), many)

    def qk(s):
        scores[lax.rem(s, LEAD + 1)] = dot(q_all[step_rows(s), :].astype(BF16), k_v[lax.rem(s, SLOTS)]) * scale

    def weights_of(s):
        t = scores[lax.rem(s, LEAD + 1)]
        e = jnp.exp(t - jnp.max(t, -1, keepdims=True))
        return (e * (1.0 / jnp.sum(e, -1, keepdims=True))).astype(BF16)

    def pv(s, w):
        o = dot_t(w, v_v[lax.rem(s, SLOTS)])
        start = place(iota((many, 1), 0))
        o = jnp.where((col >= start) & (col < start + HEAD), o, 0.0)
        o = o[:, : fold // 2] + o[:, fold // 2 :]
        o = o + pltpu.roll(o, fold // 4, axis=1)
        seen_all[s] = o[:GROUP, :wide] + o[GROUP:, :wide]

    def keys_in(s):
        return fetch(s, k_hbm, k_v, sem_k)

    def values_in(s):
        return fetch(s, v_hbm, v_v, sem_v)

    def attention(s):
        keys_in(s + LEAD).wait()
        values_in(s).wait()
        w = weights_of(s)
        qk(s + LEAD)
        pv(s, w)

        @pl.when(s + LEAD + SLOTS < steps)
        def _():
            keys_in(s + LEAD + SLOTS).start(priority=1)

        @pl.when(s + SLOTS < steps)
        def _():
            values_in(s + SLOTS).start(priority=1)

    def project(c):
        seen = jnp.concatenate([seen_all[c * per + i] for i in range(per)], 0).astype(BF16)
        cut(dot(seen, wo_v[...]), [c], t1)
        scatter(t1.at[c], r1.at[c], (s1.at[c], q1.at[c]))

    def states(c):
        xblock(c).wait()
        landed(r1.at[c], q1.at[c])
        h_all[c, me] = total(xb_v[c].astype(F32), t1.at[c], r1.at[c])
        for p in peers:
            send(h_all.at[c, me], h_all.at[c, me], (sh.at[c], qh.at[c]), p)

    def states_of(c):
        landed(r1.at[c], qh.at[c])
        return [jnp.concatenate([h_all[c, i * cg + j].astype(F32) for j in range(cg)], 1) for i in range(2)]

    def mlp(h):
        b = normed(jnp.concatenate(h, 0), gain_of(gm_v))
        gate = dot(b, wg_v[...])
        up = dot(b, wu_v[...])
        return dot((jax.nn.silu(gate) * up).astype(BF16), wd_v[...])

    def spread_half(z, parts, buf, sems, phase):
        for i in range(2):
            axis = (i + phase) % 2
            buf[z, i, my[axis]] = parts[i].astype(BF16)
        for step in sorted(range(1, side), key=lambda k: -away[k]):
            for i in range(2):
                axis = (i + phase) % 2
                there = lax.rem(my[axis] + step, side)
                peer = there * side + my[1] if axis == 0 else my[0] * side + there
                slot = buf.at[z, i, my[axis]]
                send(slot, slot, (sems[0].at[z], sems[1].at[z]), peer)

    def halves(term):
        return term[:, : d // 2], term[:, d // 2 :]

    def gathered(z, buf, sems):
        landed(buf.at[z, :, 0 : side - 1], sems[1].at[z])
        out = []
        for i in range(2):
            acc = buf[z, i, 0].astype(F32)
            for k in range(1, side):
                acc = acc + buf[z, i, k].astype(F32)
            out.append(acc)
        return out

    def project_part(z):
        s = steps - per + z * (per // 2)
        seen = jnp.concatenate([seen_all[s + i] for i in range(per // 2)], 0).astype(BF16)
        spread_half(z, halves(dot(seen, wo_v[...])), a1, (sa1, qa1), 0)

    def states_part(z):
        first = (chunks * rows) + z * small
        h = x_v[first : first + small, :].astype(F32) + jnp.concatenate(gathered(z, b1, (sb1, qb1)), 1)
        h_part[z] = h.astype(BF16)

    def outputs_part(z):
        y = h_part[z].astype(F32) + jnp.concatenate(gathered(z, b2, (sb2, qb2)), 1)
        y_hbm[2 * chunks + z] = y.astype(BF16)

    def scatter2(c):
        scatter(t2.at[c], r2.at[c], (s2.at[c], q2.at[c]))

    def outputs(c):
        landed(r2.at[c], q2.at[c])
        ys[c] = total(h_all[c, me].astype(F32), t2.at[c], r2.at[c])
        pltpu.make_async_copy(ys.at[c], block_of(y_hbm, c), sem_y.at[c]).start()
        for p in peers:
            send(ys.at[c], block_of(y_hbm, c), (sy.at[c], qy.at[c]), p)

    def between(s):
        @pl.when(s == steps - SLOTS - 1)
        def _():
            for i in range(1, len(weights)):
                weight(i).start(priority=1)

        @pl.when(s == per - 1)
        def _():
            weight(0).wait()
            pl.semaphore_wait(barrier, n - 1)

        @pl.when(lax.rem(s, per) == per - 1)
        def _():
            project(lax.div(s, per))

        @pl.when(s == steps - per // 2 - 1)
        def _():
            project_part(0)

        @pl.when((s >= per) & (s < steps - per) & (lax.rem(s, per) == per - 2))
        def _():
            states(lax.div(s, per) - 1)

    def body(s, carry):
        attention(s)
        between(s)
        return carry

    for s in range(LEAD):
        keys_in(s).wait()
        qk(s)
        keys_in(s + SLOTS).start(priority=1)
    lax.fori_loop(0, steps - LEAD, body, 0)
    for s in range(steps - LEAD, steps):
        w = weights_of(s)
        values_in(s).wait()
        pv(s, w)
    project_part(1)
    spread_half(0, gathered(0, a1, (sa1, qa1)), b1, (sb1, qb1), 1)
    states(chunks - 1)
    first[4].wait()
    for i in range(1, len(weights)):
        weight(i).wait()
    cut(mlp([h for c in range(chunks - 1) for h in states_of(c)]), range(chunks - 1), t2)
    spread_half(1, gathered(1, a1, (sa1, qa1)), b1, (sb1, qb1), 1)
    for c in range(chunks - 1):
        scatter2(c)
    states_part(0)
    term = mlp([*states_of(chunks - 1), h_part[0].astype(F32)])
    cut(term[:rows], [chunks - 1], t2)
    scatter2(chunks - 1)
    spread_half(0, halves(term[rows:]), a2, (sa2, qa2), 0)
    states_part(1)
    spread_half(1, halves(mlp([h_part[1].astype(F32)])), a2, (sa2, qa2), 0)
    for c in range(chunks - 1):
        outputs(c)
    spread_half(0, gathered(0, a2, (sa2, qa2)), b2, (sb2, qb2), 1)
    outputs(chunks - 1)
    spread_half(1, gathered(1, a2, (sa2, qa2)), b2, (sb2, qb2), 1)
    outputs_part(0)
    outputs_part(1)

    for z in range(2):
        for sem in (sa1, sb1, sa2, sb2):
            landed(a1.at[z, :, 0 : side - 1], sem.at[z])
    for c in range(chunks):
        landed(r1.at[c], s1.at[c])
        landed(r1.at[c], sh.at[c])
        landed(r1.at[c], s2.at[c])
        landed(r1.at[c], sy.at[c])
        landed(r1.at[c], qy.at[c])
        pltpu.make_async_copy(ys.at[c], block_of(y_hbm, c), sem_y.at[c]).wait()


def solution(mesh):
    n = mesh.shape["tp"]

    def step(x, k_cache, v_cache, gain_a, wq, wo, gain_m, w_gate, w_up, w_down):
        batch, cache, heads, head = k_cache.shape
        d, wide = wq.shape
        ff = w_gate.shape[1]
        fold = GROUP * wide
        rows = batch // QUARTER
        chunks = QUARTER - 1
        block = (rows // 2, d // (n // 2))
        keys = jnp.transpose(k_cache, (0, 2, 3, 1)).reshape(batch * wide, cache)
        values = jnp.transpose(v_cache, (0, 2, 3, 1)).reshape(batch * wide, cache)
        half = head // 2
        angle = (cache - 1) * float(THETA) ** (-np.arange(half) / half)
        cos, sin = np.cos(angle), np.sin(angle)
        turn = np.stack([np.tile([*cos, *cos], fold // head), np.tile([*-sin, *sin], fold // head)]).astype(np.float32)
        hbm = pl.BlockSpec(memory_space=pltpu.HBM)
        gains = (d // 128, 128)
        dma, per_chunk = pltpu.SemaphoreType.DMA, pltpu.SemaphoreType.DMA((chunks,))
        return pl.pallas_call(
            functools.partial(kernel, n),
            out_shape=pltpu.VMEM((batch // block[0], block[0], d), BF16),
            in_specs=[hbm] * 11,
            out_specs=pl.BlockSpec(memory_space=pltpu.VMEM),
            scratch_shapes=[
                pltpu.VMEM((batch, d), BF16),
                pltpu.VMEM(gains, BF16),
                pltpu.VMEM(gains, BF16),
                pltpu.VMEM((2, fold), F32),
                pltpu.VMEM((wide, d), BF16),
                pltpu.VMEM((wide, d), BF16),
                pltpu.VMEM((d, ff), BF16),
                pltpu.VMEM((d, ff), BF16),
                pltpu.VMEM((ff, d), BF16),
                pltpu.VMEM((SLOTS, fold, cache), BF16),
                pltpu.VMEM((SLOTS, fold, cache), BF16),
                pltpu.VMEM((batch * heads, fold), F32),
                pltpu.VMEM((LEAD + 1, GROUP * heads, cache), F32),
                pltpu.VMEM((batch // GROUP, GROUP, wide), F32),
                pltpu.VMEM((chunks, *block), BF16),
                pltpu.VMEM((chunks, n, *block), BF16),
                pltpu.VMEM((chunks, n - 1, *block), BF16),
                pltpu.VMEM((chunks, n, *block), BF16),
                pltpu.VMEM((chunks, n, *block), BF16),
                pltpu.VMEM((chunks, n - 1, *block), BF16),
                pltpu.VMEM((chunks, *block), BF16),
                *[pltpu.VMEM((2, 2, math.isqrt(n), rows // 2, d // 2), BF16)] * 4,
                pltpu.VMEM((2, rows // 2, d), BF16),
                dma((5,)), dma((4,)), dma((SLOTS,)), dma((SLOTS,)), per_chunk, per_chunk,
                *[per_chunk] * 8, *[dma((2,))] * 8,
            ],
            compiler_params=pltpu.CompilerParams(
                collective_id=0, has_side_effects=True, vmem_limit_bytes=60 * 2**20
            ),
        )(x, keys, values, gain_a.reshape(gains), wq.T, wo, gain_m.reshape(gains), w_gate, w_up, w_down, turn).reshape(x.shape)

    states, cache, columns, rows_of = P("dp", None), P("dp", None, "tp", None), P(None, "tp"), P("tp", None)
    return jax.shard_map(
        step,
        mesh=mesh,
        in_specs=(states, cache, cache, P(None), columns, rows_of, P(None), columns, columns, rows_of),
        out_specs=states,
        check_vma=False,
    )
```

```python
import functools
import math

import jax
import jax.numpy as jnp
import numpy as np
from jax import lax
from jax.experimental import pallas as pl
from jax.experimental.pallas import tpu as pltpu
from jax.sharding import PartitionSpec as P

HEAD = 96
THETA = 10000
GROUP = 4
QUARTER = 4
LEAD = 1
SLOTS = 4
MESH = pl.DeviceIdType.MESH
F32, BF16 = jnp.float32, jnp.bfloat16


def dot(a, b):
    return jnp.dot(a, b, preferred_element_type=F32)


def dot_t(a, b):
    return lax.dot_general(a, b, (((1,), (1,)), ((), ())), preferred_element_type=F32)


def normed(wide, gain):
    scale = lax.rsqrt(jnp.mean(wide * wide, -1, keepdims=True) + 1e-6)
    return (wide * scale * gain).astype(BF16)


def iota(shape, axis):
    return lax.broadcasted_iota(jnp.int32, shape, axis)


def ones_where(mask):
    return jnp.where(mask, 1.0, 0.0).astype(BF16)


def kernel(
    n, x_hbm, k_hbm, v_hbm, ga_hbm, wq_hbm, wo_hbm, gm_hbm, wg_hbm, wu_hbm, wd_hbm, cs_hbm,
    y_hbm,
    x_v, ga_v, gm_v, cs_v, wq_v, wo_v, wg_v, wu_v, wd_v, k_v, v_v, q_all, scores, seen_all, xb_v,
    t1, r1, h_all, t2, r2, ys, a1, b1, a2, b2, h_part,
    sem_i, sem_w, sem_k, sem_v, sem_b, sem_y, s1, q1, sh, qh, s2, q2, sy, qy,
    sa1, qa1, sb1, qb1, sa2, qa2, sb2, qb2,
):
    batch, d = x_hbm.shape
    steps = batch // GROUP
    rows = batch // QUARTER
    per = steps // QUARTER
    chunks = QUARTER - 1
    small = rows // 2
    wide = wq_hbm.shape[0]
    heads = wide // HEAD
    fold = GROUP * wide
    rh = rows // 2
    cg = n // 2
    cw = d // cg
    scale = HEAD**-0.5
    me = lax.axis_index("tp")
    mr, mc = lax.div(me, cg), lax.rem(me, cg)

    side = math.isqrt(n)
    my = (lax.div(me, side), lax.rem(me, side))
    away = [min(i, side - i) for i in range(side)]
    moves = sorted(
        ((i, j) for i in range(side) for j in range(side) if i + j), key=lambda m: (-away[m[0]] - away[m[1]], m)
    )
    peers = [
        lax.rem(lax.div(me, side) + i, side) * side + lax.rem(lax.rem(me, side) + j, side) for i, j in moves
    ]

    first = [
        pltpu.make_async_copy(a, b, sem_i.at[i])
        for i, (a, b) in enumerate([(x_hbm, x_v), (ga_hbm, ga_v), (wq_hbm, wq_v), (cs_hbm, cs_v), (gm_hbm, gm_v)])
    ]
    for copy in first:
        copy.start()
    weights = [(wo_hbm, wo_v), (wg_hbm, wg_v), (wu_hbm, wu_v), (wd_hbm, wd_v)]

    def weight(i):
        return pltpu.make_async_copy(*weights[i], sem_w.at[i])

    def block_of(ref, c):
        return ref.at[2 * c + mr, :, pl.ds(pl.multiple_of(cw * mc, 128), cw)]

    x_rows = x_hbm.reshape(batch // rh, rh, d)

    def xblock(c):
        return pltpu.make_async_copy(block_of(x_rows, c), xb_v.at[c], sem_b.at[c])

    def fetch(s, src, dst, sem):
        slot = lax.rem(s, SLOTS)
        return pltpu.make_async_copy(
            src.at[pl.ds(pl.multiple_of(s * fold, fold), fold)], dst.at[slot], sem.at[slot]
        )

    for s in range(SLOTS + LEAD):
        if s < SLOTS:
            fetch(s, k_hbm, k_v, sem_k).start(priority=1)
        if s >= LEAD:
            fetch(s - LEAD, v_hbm, v_v, sem_v).start(priority=1)
    for c in range(chunks):
        xblock(c).start(priority=1)
    weight(0).start(priority=1)

    barrier = pltpu.get_barrier_semaphore()
    for p in peers:
        pl.semaphore_signal(barrier, inc=1, device_id={"tp": p}, device_id_type=MESH)

    col = iota((1, fold), 1)
    inner = col
    for i in range(1, GROUP):
        inner = inner - jnp.where(col >= i * wide, wide, 0)
    within = inner
    for i in range(1, heads):
        within = within - jnp.where(inner >= i * HEAD, HEAD, 0)
    half = HEAD // 2
    partner = jnp.where(within < half, inner + half, inner - half)
    row = iota((wide, fold), 0)
    tile_m, swap_m = ones_where(row == inner), ones_where(row == partner)

    def place(r):
        return lax.rem(r, GROUP) * wide + lax.div(r, GROUP) * HEAD

    def gain_of(ref):
        g = ref[...].astype(F32)
        return jnp.concatenate([g[i : i + 1] for i in range(g.shape[0])], 1)

    with jax.named_scope("first"):
        first[0].wait()
    with jax.named_scope("first"):
        first[1].wait()
    a = normed(x_v[...].astype(F32), gain_of(ga_v))
    with jax.named_scope("first"):
        first[2].wait()
    q = dot_t(a, wq_v[...]).astype(BF16)
    with jax.named_scope("first"):
        first[3].wait()
    turned = (dot(q, tile_m) * cs_v[0:1] + dot(q, swap_m) * cs_v[1:2]).astype(BF16)
    many = GROUP * heads
    r = iota((batch * heads, batch), 0)
    spread = ones_where(lax.div(r, many) * GROUP + lax.rem(r, GROUP) == iota((batch * heads, batch), 1))
    at = place(lax.rem(iota((batch * heads, 1), 0), many))
    q_all[...] = jnp.where((col >= at) & (col < at + HEAD), dot(spread, turned), 0.0)

    def send(src, dst, sems, peer):
        pltpu.make_async_remote_copy(
            src_ref=src, dst_ref=dst, send_sem=sems[0], recv_sem=sems[1],
            device_id={"tp": peer}, device_id_type=MESH,
        ).start()

    def landed(ref, sem):
        pltpu.make_async_copy(ref, ref, sem).wait()

    def cut(term, cs, t):
        for a, c in enumerate(cs):
            for o in range(n):
                i = a * rows + o // cg * rh
                t[c, o] = term[i : i + rh, o % cg * cw : (o % cg + 1) * cw].astype(BF16)

    def scatter(t, r, sems):
        for k, p in enumerate(peers):
            send(t.at[p], r.at[k], sems, p)

    def total(first, t, r):
        acc = t[me].astype(F32)
        for k in range(n - 1):
            acc = acc + r[k].astype(F32)
        return (first + acc).astype(BF16)

    def step_rows(s):
        return pl.ds(pl.multiple_of(s * many, many), many)

    def qk(s):
        scores[lax.rem(s, LEAD + 1)] = dot(q_all[step_rows(s), :].astype(BF16), k_v[lax.rem(s, SLOTS)]) * scale

    def weights_of(s):
        t = scores[lax.rem(s, LEAD + 1)]
        e = jnp.exp(t - jnp.max(t, -1, keepdims=True))
        return (e * (1.0 / jnp.sum(e, -1, keepdims=True))).astype(BF16)

    def pv(s, w):
        o = dot_t(w, v_v[lax.rem(s, SLOTS)])
        start = place(iota((many, 1), 0))
        o = jnp.where((col >= start) & (col < start + HEAD), o, 0.0)
        o = o[:, : fold // 2] + o[:, fold // 2 :]
        o = o + pltpu.roll(o, fold // 4, axis=1)
        seen_all[s] = o[:GROUP, :wide] + o[GROUP:, :wide]

    def keys_in(s):
        return fetch(s, k_hbm, k_v, sem_k)

    def values_in(s):
        return fetch(s, v_hbm, v_v, sem_v)

    def attention(s):
        keys_in(s + LEAD).wait()
        values_in(s).wait()
        w = weights_of(s)
        qk(s + LEAD)
        pv(s, w)

        @pl.when(s + LEAD + SLOTS < steps)
        def _():
            keys_in(s + LEAD + SLOTS).start(priority=1)

        @pl.when(s + SLOTS < steps)
        def _():
            values_in(s + SLOTS).start(priority=1)

    def project(c):
        seen = jnp.concatenate([seen_all[c * per + i] for i in range(per)], 0).astype(BF16)
        cut(dot(seen, wo_v[...]), [c], t1)
        with jax.named_scope("scatter"):
            scatter(t1.at[c], r1.at[c], (s1.at[c], q1.at[c]))

    def states(c):
        xblock(c).wait()
        with jax.named_scope("landed"):
            landed(r1.at[c], q1.at[c])
        h_all[c, me] = total(xb_v[c].astype(F32), t1.at[c], r1.at[c])
        for p in peers:
            send(h_all.at[c, me], h_all.at[c, me], (sh.at[c], qh.at[c]), p)

    def states_of(c):
        with jax.named_scope("landed"):
            landed(r1.at[c], qh.at[c])
        return [jnp.concatenate([h_all[c, i * cg + j].astype(F32) for j in range(cg)], 1) for i in range(2)]

    def mlp(h):
        b = normed(jnp.concatenate(h, 0), gain_of(gm_v))
        gate = dot(b, wg_v[...])
        up = dot(b, wu_v[...])
        return dot((jax.nn.silu(gate) * up).astype(BF16), wd_v[...])

    def spread_half(z, parts, buf, sems, phase):
        for i in range(2):
            axis = (i + phase) % 2
            buf[z, i, my[axis]] = parts[i].astype(BF16)
        for step in sorted(range(1, side), key=lambda k: -away[k]):
            for i in range(2):
                axis = (i + phase) % 2
                there = lax.rem(my[axis] + step, side)
                peer = there * side + my[1] if axis == 0 else my[0] * side + there
                slot = buf.at[z, i, my[axis]]
                send(slot, slot, (sems[0].at[z], sems[1].at[z]), peer)

    def halves(term):
        return term[:, : d // 2], term[:, d // 2 :]

    def gathered(z, buf, sems):
        with jax.named_scope("landed"):
            landed(buf.at[z, :, 0 : side - 1], sems[1].at[z])
        out = []
        for i in range(2):
            acc = buf[z, i, 0].astype(F32)
            for k in range(1, side):
                acc = acc + buf[z, i, k].astype(F32)
            out.append(acc)
        return out

    def project_part(z):
        s = steps - per + z * (per // 2)
        seen = jnp.concatenate([seen_all[s + i] for i in range(per // 2)], 0).astype(BF16)
        with jax.named_scope("spread_half"):
            spread_half(z, halves(dot(seen, wo_v[...])), a1, (sa1, qa1), 0)

    def states_part(z):
        first = (chunks * rows) + z * small
        h = x_v[first : first + small, :].astype(F32) + jnp.concatenate(gathered(z, b1, (sb1, qb1)), 1)
        h_part[z] = h.astype(BF16)

    def outputs_part(z):
        y = h_part[z].astype(F32) + jnp.concatenate(gathered(z, b2, (sb2, qb2)), 1)
        y_hbm[2 * chunks + z] = y.astype(BF16)

    def scatter2(c):
        with jax.named_scope("scatter"):
            scatter(t2.at[c], r2.at[c], (s2.at[c], q2.at[c]))

    def outputs(c):
        with jax.named_scope("landed"):
            landed(r2.at[c], q2.at[c])
        ys[c] = total(h_all[c, me].astype(F32), t2.at[c], r2.at[c])
        pltpu.make_async_copy(ys.at[c], block_of(y_hbm, c), sem_y.at[c]).start()
        for p in peers:
            send(ys.at[c], block_of(y_hbm, c), (sy.at[c], qy.at[c]), p)

    def between(s):
        @pl.when(s == steps - SLOTS - 1)
        def _():
            for i in range(1, len(weights)):
                weight(i).start(priority=1)

        @pl.when(s == per - 1)
        def _():
            with jax.named_scope("weight"):
                weight(0).wait()
            with jax.named_scope("barrier"):
                pl.semaphore_wait(barrier, n - 1)

        @pl.when(lax.rem(s, per) == per - 1)
        def _():
            with jax.named_scope("project"):
                project(lax.div(s, per))

        @pl.when(s == steps - per // 2 - 1)
        def _():
            with jax.named_scope("project_part"):
                project_part(0)

        @pl.when((s >= per) & (s < steps - per) & (lax.rem(s, per) == per - 2))
        def _():
            with jax.named_scope("states"):
                states(lax.div(s, per) - 1)

    def body(s, carry):
        with jax.named_scope("attention"):
            attention(s)
        between(s)
        return carry

    for s in range(LEAD):
        keys_in(s).wait()
        qk(s)
        keys_in(s + SLOTS).start(priority=1)
    lax.fori_loop(0, steps - LEAD, body, 0)
    for s in range(steps - LEAD, steps):
        w = weights_of(s)
        values_in(s).wait()
        pv(s, w)
    with jax.named_scope("project_part"):
        project_part(1)
    with jax.named_scope("spread_half"):
        spread_half(0, gathered(0, a1, (sa1, qa1)), b1, (sb1, qb1), 1)
    with jax.named_scope("states"):
        states(chunks - 1)
    with jax.named_scope("first"):
        first[4].wait()
    for i in range(1, len(weights)):
        with jax.named_scope("weight"):
            weight(i).wait()
    cut(mlp([h for c in range(chunks - 1) for h in states_of(c)]), range(chunks - 1), t2)
    with jax.named_scope("spread_half"):
        spread_half(1, gathered(1, a1, (sa1, qa1)), b1, (sb1, qb1), 1)
    for c in range(chunks - 1):
        with jax.named_scope("scatter2"):
            scatter2(c)
    with jax.named_scope("states_part"):
        states_part(0)
    term = mlp([*states_of(chunks - 1), h_part[0].astype(F32)])
    cut(term[:rows], [chunks - 1], t2)
    with jax.named_scope("scatter2"):
        scatter2(chunks - 1)
    with jax.named_scope("spread_half"):
        spread_half(0, halves(term[rows:]), a2, (sa2, qa2), 0)
    with jax.named_scope("states_part"):
        states_part(1)
    with jax.named_scope("spread_half"):
        spread_half(1, halves(mlp([h_part[1].astype(F32)])), a2, (sa2, qa2), 0)
    for c in range(chunks - 1):
        with jax.named_scope("outputs"):
            outputs(c)
    with jax.named_scope("spread_half"):
        spread_half(0, gathered(0, a2, (sa2, qa2)), b2, (sb2, qb2), 1)
    with jax.named_scope("outputs"):
        outputs(chunks - 1)
    with jax.named_scope("spread_half"):
        spread_half(1, gathered(1, a2, (sa2, qa2)), b2, (sb2, qb2), 1)
    with jax.named_scope("outputs_part"):
        outputs_part(0)
    with jax.named_scope("outputs_part"):
        outputs_part(1)

    for z in range(2):
        for sem in (sa1, sb1, sa2, sb2):
            with jax.named_scope("landed"):
                landed(a1.at[z, :, 0 : side - 1], sem.at[z])
    for c in range(chunks):
        with jax.named_scope("landed"):
            landed(r1.at[c], s1.at[c])
        with jax.named_scope("landed"):
            landed(r1.at[c], sh.at[c])
        with jax.named_scope("landed"):
            landed(r1.at[c], s2.at[c])
        with jax.named_scope("landed"):
            landed(r1.at[c], sy.at[c])
        with jax.named_scope("landed"):
            landed(r1.at[c], qy.at[c])
        pltpu.make_async_copy(ys.at[c], block_of(y_hbm, c), sem_y.at[c]).wait()


def solution(mesh):
    n = mesh.shape["tp"]

    def step(x, k_cache, v_cache, gain_a, wq, wo, gain_m, w_gate, w_up, w_down):
        batch, cache, heads, head = k_cache.shape
        d, wide = wq.shape
        ff = w_gate.shape[1]
        fold = GROUP * wide
        rows = batch // QUARTER
        chunks = QUARTER - 1
        block = (rows // 2, d // (n // 2))
        keys = jnp.transpose(k_cache, (0, 2, 3, 1)).reshape(batch * wide, cache)
        values = jnp.transpose(v_cache, (0, 2, 3, 1)).reshape(batch * wide, cache)
        half = head // 2
        angle = (cache - 1) * float(THETA) ** (-np.arange(half) / half)
        cos, sin = np.cos(angle), np.sin(angle)
        turn = np.stack([np.tile([*cos, *cos], fold // head), np.tile([*-sin, *sin], fold // head)]).astype(np.float32)
        hbm = pl.BlockSpec(memory_space=pltpu.HBM)
        gains = (d // 128, 128)
        dma, per_chunk = pltpu.SemaphoreType.DMA, pltpu.SemaphoreType.DMA((chunks,))
        return pl.pallas_call(
            functools.partial(kernel, n),
            out_shape=pltpu.VMEM((batch // block[0], block[0], d), BF16),
            in_specs=[hbm] * 11,
            out_specs=pl.BlockSpec(memory_space=pltpu.VMEM),
            scratch_shapes=[
                pltpu.VMEM((batch, d), BF16),
                pltpu.VMEM(gains, BF16),
                pltpu.VMEM(gains, BF16),
                pltpu.VMEM((2, fold), F32),
                pltpu.VMEM((wide, d), BF16),
                pltpu.VMEM((wide, d), BF16),
                pltpu.VMEM((d, ff), BF16),
                pltpu.VMEM((d, ff), BF16),
                pltpu.VMEM((ff, d), BF16),
                pltpu.VMEM((SLOTS, fold, cache), BF16),
                pltpu.VMEM((SLOTS, fold, cache), BF16),
                pltpu.VMEM((batch * heads, fold), F32),
                pltpu.VMEM((LEAD + 1, GROUP * heads, cache), F32),
                pltpu.VMEM((batch // GROUP, GROUP, wide), F32),
                pltpu.VMEM((chunks, *block), BF16),
                pltpu.VMEM((chunks, n, *block), BF16),
                pltpu.VMEM((chunks, n - 1, *block), BF16),
                pltpu.VMEM((chunks, n, *block), BF16),
                pltpu.VMEM((chunks, n, *block), BF16),
                pltpu.VMEM((chunks, n - 1, *block), BF16),
                pltpu.VMEM((chunks, *block), BF16),
                *[pltpu.VMEM((2, 2, math.isqrt(n), rows // 2, d // 2), BF16)] * 4,
                pltpu.VMEM((2, rows // 2, d), BF16),
                dma((5,)), dma((4,)), dma((SLOTS,)), dma((SLOTS,)), per_chunk, per_chunk,
                *[per_chunk] * 8, *[dma((2,))] * 8,
            ],
            compiler_params=pltpu.CompilerParams(
                collective_id=0, has_side_effects=True, vmem_limit_bytes=60 * 2**20
            ),
        )(x, keys, values, gain_a.reshape(gains), wq.T, wo, gain_m.reshape(gains), w_gate, w_up, w_down, turn).reshape(x.shape)

    states, cache, columns, rows_of = P("dp", None), P("dp", None, "tp", None), P(None, "tp"), P("tp", None)
    return jax.shard_map(
        step,
        mesh=mesh,
        in_specs=(states, cache, cache, P(None), columns, rows_of, P(None), columns, columns, rows_of),
        out_specs=states,
        check_vma=False,
    )
```
